32 devices in a mesh: tier: 4 (over y, core), mode: 8 (over z, x).
Axes of the slice: x: 2, y: 2, z: 4, core: 2. Of those that a mesh axis runs over, the one named last changes fastest.
Arguments:
- ados: float32 [4, 8, 2, 2, 9216], P('tier', 'mode'), may hold values from -6 to 6
- hamiltonian: float32 [96, 96], replicated, may hold values from -0.3125 to 0.3125
- couplings: float32 [16, 96], replicated, may hold values from -2.4 to 2.4
- rates: float32 [16], replicated, may hold values from 0.05 to 0.6
- strength: float32 [2, 16], replicated, may hold values from -1.8 to 1.8
- occupancy: int32 [4, 8, 2, 16], P('tier', 'mode'), may hold values from 0 to 8, as said below
- up_index: int32 [4, 8, 2, 16], P('tier', 'mode'), may hold values from 0 to 8, as said below
- down_index: int32 [4, 8, 2, 16], P('tier', 'mode'), may hold values from 0 to 8, as said below
Outputs:
- evolved: float32 [4, 8, 2, 2, 9216], P('tier', 'mode')
The draws below stay inside these ranges and needn't reach their ends.
Inputs may be any that keep to these rules, and one draw needn't show every extreme that they name: `occupancy`: each matrix is occupied in at most 8 quanta in all, summed over the 16 modes; higher tier bins hold matrices of higher tiers on average. For each mode, up_index and down_index describe the same pairs in the two directions: if the entry of matrix a for mode k in up_index names matrix b, then the entry of b for mode k in down_index names a, and the reverse; no matrix is named twice for one mode. The value 4 * 2 names no matrix, and no entry names a tier outside the hierarchy. `down_index`: see up_index.
All inputs are finite; a program needn't handle non-finite values.
Results may differ from the reference program's by a relative error of at most 0.00005.
Values sent between devices are 32-bit elements; how exact they have to be, the bound alone decides.
No kernel may reach another device: no remote copies, remote signals or barrier semaphores. Data moves between devices by JAX's collectives and lax.ppermute only.
A program may use at most 64 MiB of HBM per device.

```python
import math
import jax
import jax.numpy as jnp
from jax import lax

D = 96
K = 16
DEPTH = 8
A_DEV = 2
TIER_BINS = 4
MODE_BINS = 8


def coupling_tables(key):
    base = jax.random.fold_in(key, 7)
    key_class, key_order, key_shift, key_turn = jax.random.split(base, 4)
    classes = jax.random.randint(key_class, (K, A_DEV), 0, 5)
    scores = jax.random.randint(key_order, (K, A_DEV), 0, 1 << 20) * A_DEV + jnp.arange(A_DEV)[None, :]
    order = jnp.argsort(scores, axis=1)
    inverse = jnp.argsort(order, axis=1)
    shifts = jax.random.randint(key_shift, (K, TIER_BINS, MODE_BINS), 0, A_DEV)
    turns = jax.random.randint(key_turn, (K, TIER_BINS, MODE_BINS), 0, A_DEV)
    return (classes, order, inverse, shifts, turns)


def draw_down_index(key, part):
    classes, order, inverse, shifts, turns = coupling_tables(key)
    tier_pos = jnp.arange(TIER_BINS)[:, None, None, None]
    mode_pos = jnp.arange(MODE_BINS)[None, :, None, None]
    slot_pos = jnp.arange(A_DEV)[None, None, :, None]
    mode_key = jnp.arange(K)[None, None, None, :]
    turn_now = turns[mode_key, tier_pos, mode_pos]
    rotated = order[mode_key, (slot_pos - turn_now) % A_DEV]
    kind = classes[mode_key, rotated]
    source_tier = tier_pos - kind % 2
    source_mode = (mode_pos - kind // 2) % MODE_BINS
    living = (kind < 4) & (source_tier >= 0)
    shift_now = shifts[mode_key, jnp.clip(source_tier, 0, TIER_BINS - 1), source_mode]
    source_slot = (rotated - shift_now) % A_DEV
    return jnp.where(living, kind * A_DEV + source_slot, 4 * A_DEV).astype(jnp.int32)


def draw_up_index(key, part):
    classes, order, inverse, shifts, turns = coupling_tables(key)
    tier_pos = jnp.arange(TIER_BINS)[:, None, None, None]
    mode_pos = jnp.arange(MODE_BINS)[None, :, None, None]
    slot_pos = jnp.arange(A_DEV)[None, None, :, None]
    mode_key = jnp.arange(K)[None, None, None, :]
    shift_now = shifts[mode_key, tier_pos, mode_pos]
    rotated = (slot_pos + shift_now) % A_DEV
    kind = classes[mode_key, rotated]
    target_tier = tier_pos + kind % 2
    target_mode = (mode_pos + kind // 2) % MODE_BINS
    living = (kind < 4) & (target_tier < TIER_BINS)
    turn_now = turns[mode_key, jnp.clip(target_tier, 0, TIER_BINS - 1), target_mode]
    target_slot = (inverse[mode_key, rotated] + turn_now) % A_DEV
    return jnp.where(living, kind * A_DEV + target_slot, 4 * A_DEV).astype(jnp.int32)


def draw_occupancy(key, part):
    base = jax.random.fold_in(key, 3)
    key_pick, key_live = jax.random.split(base, 2)
    picks = jax.random.randint(key_pick, (TIER_BINS, MODE_BINS, A_DEV, DEPTH), 0, K)
    tier_pos = jnp.arange(TIER_BINS)[:, None, None, None]
    slot_pos = jnp.arange(A_DEV)[None, None, :, None]
    chance = jax.random.randint(key_live, (TIER_BINS, MODE_BINS, A_DEV, DEPTH), 0, TIER_BINS + 1)
    living = chance <= tier_pos + 1
    filled = (tier_pos == TIER_BINS - 1) & (slot_pos == 0)
    filled = jnp.broadcast_to(filled, picks.shape)
    picks = jnp.where(filled, jnp.broadcast_to(picks[..., :1], picks.shape), picks)
    living = living | filled
    picks = jnp.where(living, picks, K)
    counts = jnp.sum((picks[..., None] == jnp.arange(K)[None, None, None, None, :]).astype(jnp.int32), axis=3)
    return counts.astype(jnp.int32)


def levels(own_key, extent, shards, low, high):
    loudness, own = 1.0, jax.random.fold_in(own_key, 6)
    for axis_at, blocks in shards:
        steps = jnp.exp(jax.random.uniform(jax.random.fold_in(own, axis_at), (blocks,), jnp.float32, low / len(shards), high / len(shards)))
        loudness = loudness * jnp.repeat(steps, extent[axis_at] // blocks).reshape([-1 if axis == axis_at else 1 for axis in range(len(extent))])
    return loudness


def scatter_about(stream_key, dims, deviation, limit, shards=(), kind=jnp.bfloat16):
    drawn = jax.random.normal(stream_key, dims, jnp.float32) * deviation
    if len(shards) > 0:
        drawn = levels(stream_key, dims, shards, -0.22, 0.18) * drawn
    return jnp.clip(drawn, min=-limit, max=limit).astype(kind)


def setup_inputs(seed: int = 0) -> dict:
    splits = jax.random.split(jax.random.key(seed), 9)
    return {
        "ados": scatter_about(splits[0], (TIER_BINS, MODE_BINS, A_DEV, 2, D * D), 1.0, 6.0, ((0, 4), (1, 8)), jnp.float32),
        "hamiltonian": scatter_about(splits[1], (D, D), (4 * D) ** -0.5, 0.3125, (), jnp.float32),
        "couplings": scatter_about(splits[2], (K, D), 0.4, 2.4, (), jnp.float32),
        "rates": jnp.clip(jnp.exp(jax.random.uniform(splits[3], (K,), jnp.float32, math.log(0.05), math.log(0.6))), 0.05, 0.6),
        "strength": scatter_about(splits[4], (2, K), 0.3, 1.8, (), jnp.float32),
        "occupancy": draw_occupancy(jax.random.fold_in(splits[8], 71), 0),
        "up_index": draw_up_index(jax.random.fold_in(splits[8], 71), 0),
        "down_index": draw_down_index(jax.random.fold_in(splits[8], 71), 0),
    }


TIME_STEP = 0.3


def fetch_rows(fields, index, direction):
    tier_count = fields.shape[0]
    mode_count = fields.shape[1]
    slot_count = fields.shape[2]
    tier_pos = jnp.arange(tier_count, dtype=jnp.int32)[:, None, None]
    mode_pos = jnp.arange(mode_count, dtype=jnp.int32)[None, :, None]
    block_pos = index // slot_count
    slot_pos = index % slot_count
    tier_step = block_pos % 2
    mode_step = block_pos // 2
    source_tier = tier_pos + direction * tier_step
    source_mode = (mode_pos + direction * mode_step) % mode_count
    living = (block_pos < 4) & (source_tier >= 0) & (source_tier < tier_count)
    picked = fields[jnp.clip(source_tier, 0, tier_count - 1), source_mode, slot_pos]
    return jnp.where(living[..., None, None], picked, jnp.zeros((), jnp.float32))


def derivative(fields, ham, gaps, sums, rates, strength, occupancy, up_index, down_index):
    tier_count, mode_count, slot_count = fields.shape[0], fields.shape[1], fields.shape[2]
    sys_width = ham.shape[0]
    square = (tier_count, mode_count, slot_count, sys_width, sys_width)
    flat_shape = (tier_count, mode_count, slot_count, sys_width * sys_width)
    real_part = fields[:, :, :, 0].reshape(square)
    imag_part = fields[:, :, :, 1].reshape(square)
    highest = lax.Precision.HIGHEST
    h_real = jnp.einsum("ij,tmajk->tmaik", ham, real_part, precision=highest)
    real_h = jnp.einsum("tmaij,jk->tmaik", real_part, ham, precision=highest)
    h_imag = jnp.einsum("ij,tmajk->tmaik", ham, imag_part, precision=highest)
    imag_h = jnp.einsum("tmaij,jk->tmaik", imag_part, ham, precision=highest)
    weights = occupancy.astype(jnp.float32)
    damping = jnp.einsum("tmak,k->tma", weights, rates, precision=highest)[..., None]
    d_real = (h_imag - imag_h).reshape(flat_shape) - damping * fields[:, :, :, 0]
    d_imag = (real_h - h_real).reshape(flat_shape) - damping * fields[:, :, :, 1]

    def add_mode(which, totals):
        acc_real, acc_imag = totals
        up_rows = fetch_rows(fields, lax.dynamic_index_in_dim(up_index, which, 3, False), 1)
        down_rows = fetch_rows(fields, lax.dynamic_index_in_dim(down_index, which, 3, False), -1)
        gap_row = lax.dynamic_index_in_dim(gaps, which, 0, False)
        plus_row = lax.dynamic_index_in_dim(sums, which, 0, False)
        level = lax.dynamic_index_in_dim(weights, which, 3, True)
        real_c = strength[0, which]
        imag_c = strength[1, which]
        acc_real = acc_real + gap_row * up_rows[:, :, :, 1] + level * (
            real_c * gap_row * down_rows[:, :, :, 1] + imag_c * plus_row * down_rows[:, :, :, 0])
        acc_imag = acc_imag - gap_row * up_rows[:, :, :, 0] - level * (
            real_c * gap_row * down_rows[:, :, :, 0] - imag_c * plus_row * down_rows[:, :, :, 1])
        return acc_real, acc_imag

    d_real, d_imag = lax.fori_loop(0, gaps.shape[0], add_mode, (d_real, d_imag))
    return jnp.stack([d_real, d_imag], axis=3)


def reference(ados, hamiltonian, couplings, rates, strength, occupancy, up_index, down_index):
    ham = 0.5 * (hamiltonian + hamiltonian.T)
    mode_total = couplings.shape[0]
    gaps = (couplings[:, :, None] - couplings[:, None, :]).reshape(mode_total, -1)
    sums = (couplings[:, :, None] + couplings[:, None, :]).reshape(mode_total, -1)

    def rhs(fields):
        return derivative(fields, ham, gaps, sums, rates, strength, occupancy, up_index, down_index)

    first = rhs(ados)
    second = rhs(ados + (TIME_STEP / 2) * first)
    third = rhs(ados + (TIME_STEP / 2) * second)
    fourth = rhs(ados + TIME_STEP * third)
    return ados + (TIME_STEP / 6) * (first + 2.0 * second + 2.0 * third + fourth)
```

```python
import functools

import jax
import jax.numpy as jnp
import numpy as np
from jax import lax
from jax.experimental import pallas as pl
from jax.experimental.pallas import tpu as pltpu
from jax.sharding import PartitionSpec as P

TIME_STEP = 0.3
HIGHEST = lax.Precision.HIGHEST
AXES = ("tier", "mode")


def swap_pairs(pairs):
    return [route for a, b in pairs for route in ((a, b), (b, a))]


def routes(tiers, modes):
    def at(tier, mode):
        return tier * modes + mode % modes

    chips = tiers // 2
    core = [(at(2 * y, m), at(2 * y + 1, m)) for y in range(chips) for m in range(modes)]
    mode = [[(at(t, m), at(t, m + 1)) for t in range(tiers) for m in range(p, modes, 2)] for p in (0, 1)]
    flat, slant = [], []
    for p in (0, 1):
        lower = range(p, chips - 1, 2)
        flat.append([(at(2 * y + c, m), at(2 * y + 2 + c, m)) for y in lower for c in (0, 1) for m in range(modes)])
        slant.append([(at(2 * y + c, m), at(2 * y + 2 + c, m + 1)) for y in lower for c in (0, 1) for m in range(modes)])
    return (
        swap_pairs(core),
        [swap_pairs(r) for r in mode],
        [swap_pairs(r) for r in flat],
        [swap_pairs(r) for r in slant],
    )


def block_plan(groups, slots):
    blocks = groups * slots * 2
    rows = []
    for k in range(blocks):
        for e in range(blocks):
            d = (e + k) % blocks
            dest, source = d // 2, e // 2
            rows.append((dest, source % slots, source // slots - dest // slots, d % 2, e % 2, float(d == e)))
    return np.array(rows, np.float32)


def weights_of(plan, info, base, rise, role_up, role_down, flip, strength, slots):
    modes = strength.shape[1]
    dest = plan[:, 0].astype(np.int32)
    pick = np.eye(info.shape[0], dtype=np.float32)[dest]
    local = jnp.dot(pick, info, precision=HIGHEST)
    level, up, down = local[:, :modes], local[:, modes : 2 * modes], local[:, 2 * modes :]
    same = (plan[:, 2:3] == 0).astype(np.float32)
    name = (base + rise * (1 - same)) * slots + plan[:, 1:2]
    climb = plan[:, 2:3] * flip
    go_up = role_up * jnp.maximum(same, (climb == 1).astype(jnp.float32))
    go_down = role_down * jnp.maximum(same, (climb == -1).astype(jnp.float32))
    ups = go_up * (up == name)
    downs = go_down * (down == name) * level
    gap = ups + downs * strength[0][None, :]
    plus = downs * strength[1][None, :]
    straight = plan[:, 3:4] == plan[:, 4:5]
    sign = plan[:, 4:5] - plan[:, 3:4]
    return jnp.where(straight, plus, sign * gap), jnp.where(straight, plus, -sign * gap), level


def table_of(row_part, column_part, blocks, width):
    spread = np.kron(np.eye(blocks, dtype=np.float32), np.ones((1, width), np.float32))
    groups = row_part.shape[0] // blocks
    rows = row_part.reshape(groups, blocks, -1)
    wide = jnp.einsum("gea,el->gal", rows, spread, precision=HIGHEST)
    return wide + column_part.reshape(groups, 1, blocks * width)


def turned(value, steps, width):
    return value if steps == 0 else pltpu.roll(value, steps * width, 1)


def swapped(value):
    half = value.shape[1] // 2
    return jnp.concatenate([value[:, half:], value[:, :half]], 1)


def own_kernel(step, width, w_ref, other_ref, start_ref, near_ref, far_ref, right_ref, table_ref, out_ref, comm_ref):
    rows, lanes = w_ref.shape
    half = lanes // 2
    w = w_ref[...]
    left = jnp.dot(near_ref[...], w, precision=HIGHEST, preferred_element_type=jnp.float32)
    left += jnp.dot(far_ref[...], other_ref[...], precision=HIGHEST, preferred_element_type=jnp.float32)
    stacked = jnp.concatenate([w[:, :half], w[:, half:]], 0)
    right = jnp.dot(stacked, right_ref[...], precision=HIGHEST, preferred_element_type=jnp.float32)
    comm_ref[:, :half] = left[:, :half] - right[:rows]
    comm_ref[:, half:] = left[:, half:] - right[rows:]
    blocks = table_ref.shape[0]
    odd = (lax.broadcasted_iota(jnp.int32, (8, lanes), 1) // width) % 2 == 1
    for at in range(0, rows, 8):
        part = pl.ds(at, 8)
        value, comm = w_ref[part, :], comm_ref[part, :]
        total = None
        for k in range(blocks // 2):
            near = table_ref[k, part, :] * value
            far = table_ref[k + blocks // 2, part, :] * value
            if k == 1:
                near += jnp.where(odd, 0.0, -comm)
            if k + blocks // 2 == blocks - 1:
                far += jnp.where(odd, comm, 0.0)
            piece = turned(near + swapped(far), k, width)
            total = piece if total is None else total + piece
        out_ref[part, :] = start_ref[part, :] + step * total


def link_kernel(step, width, edges, *refs):
    part_ref, x_ref, z_ref, x_table, z_table = refs[:5]
    edge_refs = refs[5 : 5 + 4 * len(edges)]
    out_ref = refs[5 + 4 * len(edges)]
    edge_out = refs[6 + 4 * len(edges) :]
    rows, lanes = part_ref.shape
    half = lanes // 2
    blocks = x_table.shape[0]
    for at in range(0, rows, 8):
        part = pl.ds(at, 8)
        x, z = x_ref[part, :], z_ref[part, :]
        total = None
        for k in range(blocks // 2):
            near = x_table[k, part, :] * x + z_table[k, part, :] * z
            k_far = k + blocks // 2
            far = x_table[k_far, part, :] * x + z_table[k_far, part, :] * z
            piece = turned(near + swapped(far), k, width)
            total = piece if total is None else total + piece
        halves = [total[:, :half], total[:, half:]]
        for n, place in enumerate(edges):
            flat, slant, flat_table, slant_table = edge_refs[4 * n : 4 * n + 4]
            a, b = flat[part, :], slant[part, :]
            for k in range(blocks // 2):
                piece = flat_table[k, part, :] * a + slant_table[k, part, :] * b
                halves[place] = halves[place] + turned(piece, k, width)
        new = [part_ref[part, :half] + step * halves[0], part_ref[part, half:] + step * halves[1]]
        out_ref[part, :half] = new[0]
        out_ref[part, half:] = new[1]
        for n, place in enumerate(edges[: len(edge_out)]):
            edge_out[n][part, :] = new[place]


VMEM = pl.BlockSpec(memory_space=pltpu.VMEM)


def shards(tiers, modes, ados, hamiltonian, couplings, rates, strength, occupancy, up_index, down_index):
    core_route, mode_routes, flat_routes, slant_routes = routes(tiers, modes)
    slots, size = ados.shape[2], hamiltonian.shape[0]
    half, lanes = size // 2, slots * 2 * size
    tier, mode = lax.axis_index("tier"), lax.axis_index("mode")
    core, chip = tier % 2, tier // 2
    turn = chip % 2
    place = core ^ turn

    def send(value, route):
        return lax.ppermute(value, AXES, route)

    own = ados.reshape(slots * 2, size, size).transpose(1, 0, 2).reshape(size, lanes)
    keep = lax.dynamic_slice(own, (core * half, 0), (half, lanes))
    got = send(lax.dynamic_slice(own, ((1 - core) * half, 0), (half, lanes)), core_route)
    first = place == 0
    start = jnp.concatenate([jnp.where(first, keep, got), jnp.where(first, got, keep)], 1)

    facts = [a.reshape(a.shape[2:]).astype(jnp.float32) for a in (occupancy, up_index, down_index)]
    info = jnp.concatenate(facts, 1)
    other_info = send(info, core_route)
    info = jnp.concatenate([jnp.where(first, info, other_info), jnp.where(first, other_info, info)], 0)

    ham = 0.5 * (hamiltonian + hamiltonian.T)
    mine = lax.dynamic_slice(ham, (core * half, 0), (half, size))
    near = jnp.where(core == 0, mine[:, :half], mine[:, half:])
    far = jnp.where(core == 0, mine[:, half:], mine[:, :half])
    right = jnp.tile(ham, (2 * slots, 2 * slots)) * np.kron(
        np.eye(2 * slots, dtype=np.float32), np.ones((size, size), np.float32)
    )

    flip = (1 - 2 * turn).astype(jnp.float32)
    rows_c = lax.dynamic_slice(couplings, (0, core * half), (couplings.shape[0], half))
    one = jnp.float32(1.0)
    blocks = 4 * slots
    plan = block_plan(2, slots)
    sources = [(0.0, one, one)]
    for p in (0, 1):
        ahead = (mode % 2 == p).astype(jnp.float32)
        sources.append((2.0, ahead, 1.0 - ahead))
    row_w, col_w, damp = [], [], None
    for base, up, down in sources:
        a, b, level = weights_of(plan, info, base, 1.0, up, down, flip, strength, slots)
        row_w.append(a)
        col_w.append(b)
        if damp is None:
            damp = jnp.sum(level * rates[None, :], 1, keepdims=True) * plan[:, 5:6]
    row_part = jnp.dot(jnp.concatenate(row_w, 0), rows_c, precision=HIGHEST)
    row_part = jnp.concatenate([row_part[: damp.shape[0]] - damp, row_part[damp.shape[0] :]], 0)
    column_part = jnp.dot(jnp.concatenate(col_w, 0), couplings, precision=HIGHEST)
    tables = table_of(row_part, column_part, blocks, size).reshape(3, blocks, half, 2 * lanes)
    tables = [tables[0], tables[1], tables[2]]

    edge_plan = block_plan(1, slots)
    links = [p for p in (0, 1) if flat_routes[p]]
    edges = tuple(1 - p for p in links)
    edge_tables = []
    for p in links:
        lower = (chip % 2 == p) & (chip + 1 < tiers // 2)
        upper = (chip % 2 != p) & (chip >= 1)
        up, down = lower.astype(jnp.float32), upper.astype(jnp.float32)
        where = (1 - p) * slots
        pair = []
        for base in (1.0, 3.0):
            a, b, _ = weights_of(edge_plan, info[where : where + slots], base, 0.0, up, down, flip, strength, slots)
            row_part = jnp.dot(a, rows_c, precision=HIGHEST)
            column_part = jnp.dot(b, couplings, precision=HIGHEST)
            pair.append(table_of(row_part, column_part, blocks // 2, size))
        edge_tables.append(pair)

    full = jax.ShapeDtypeStruct((half, 2 * lanes), jnp.float32)
    edge = jax.ShapeDtypeStruct((half, lanes), jnp.float32)
    w = start
    brink = [start[:, q * lanes : (q + 1) * lanes] for q in edges]
    for stage in (4, 3, 2, 1):
        step = TIME_STEP / stage
        flat = [send(brink[n], flat_routes[p]) for n, p in enumerate(links)]
        slant = [send(brink[n], slant_routes[p]) for n, p in enumerate(links)]
        z = send(w, mode_routes[1])
        x = send(w, mode_routes[0])
        other = send(w, core_route)
        part = pl.pallas_call(
            functools.partial(own_kernel, step, size),
            out_shape=full,
            in_specs=[VMEM] * 7,
            out_specs=VMEM,
            scratch_shapes=[pltpu.VMEM((half, 2 * lanes), jnp.float32)],
            name="own_part",
        )(w, other, start, near, far, right, tables[0])
        extra = [a for n in range(len(links)) for a in (flat[n], slant[n], *edge_tables[n])]
        count = len(links) if stage > 1 else 0
        result = pl.pallas_call(
            functools.partial(link_kernel, step, size, edges),
            out_shape=[full] + [edge] * count,
            in_specs=[VMEM] * (5 + len(extra)),
            out_specs=[VMEM] * (1 + count),
            name="link_part",
        )(part, x, z, tables[1], tables[2], *extra)
        w, brink = result[0], result[1:]

    low, high = w[:, :lanes], w[:, lanes:]
    keep = jnp.where(first, low, high)
    got = send(jnp.where(first, high, low), core_route)
    whole = jnp.concatenate([jnp.where(core == 0, keep, got), jnp.where(core == 0, got, keep)], 0)
    return whole.reshape(size, slots * 2, size).transpose(1, 0, 2).reshape(ados.shape)


def solution(mesh):
    spread = P("tier", "mode", None, None)
    in_specs = (P("tier", "mode", None, None, None), P(), P(), P(), P(), spread, spread, spread)
    body = functools.partial(shards, mesh.shape["tier"], mesh.shape["mode"])
    return jax.shard_map(
        body, mesh=mesh, in_specs=in_specs, out_specs=P("tier", "mode", None, None, None), check_vma=False
    )
```

```python
import functools

import jax
import jax.numpy as jnp
import numpy as np
from jax import lax
from jax.experimental import pallas as pl
from jax.experimental.pallas import tpu as pltpu
from jax.sharding import PartitionSpec as P

TIME_STEP = 0.3
HIGHEST = lax.Precision.HIGHEST
AXES = ("tier", "mode")


def swap_pairs(pairs):
    return [route for a, b in pairs for route in ((a, b), (b, a))]


def routes(tiers, modes):
    def at(tier, mode):
        return tier * modes + mode % modes

    chips = tiers // 2
    core = [(at(2 * y, m), at(2 * y + 1, m)) for y in range(chips) for m in range(modes)]
    mode = [[(at(t, m), at(t, m + 1)) for t in range(tiers) for m in range(p, modes, 2)] for p in (0, 1)]
    flat, slant = [], []
    for p in (0, 1):
        lower = range(p, chips - 1, 2)
        flat.append([(at(2 * y + c, m), at(2 * y + 2 + c, m)) for y in lower for c in (0, 1) for m in range(modes)])
        slant.append([(at(2 * y + c, m), at(2 * y + 2 + c, m + 1)) for y in lower for c in (0, 1) for m in range(modes)])
    return (
        swap_pairs(core),
        [swap_pairs(r) for r in mode],
        [swap_pairs(r) for r in flat],
        [swap_pairs(r) for r in slant],
    )


def block_plan(groups, slots):
    blocks = groups * slots * 2
    rows = []
    for k in range(blocks):
        for e in range(blocks):
            d = (e + k) % blocks
            dest, source = d // 2, e // 2
            rows.append((dest, source % slots, source // slots - dest // slots, d % 2, e % 2, float(d == e)))
    return np.array(rows, np.float32)


def weights_of(plan, info, base, rise, role_up, role_down, flip, strength, slots):
    modes = strength.shape[1]
    dest = plan[:, 0].astype(np.int32)
    pick = np.eye(info.shape[0], dtype=np.float32)[dest]
    local = jnp.dot(pick, info, precision=HIGHEST)
    level, up, down = local[:, :modes], local[:, modes : 2 * modes], local[:, 2 * modes :]
    same = (plan[:, 2:3] == 0).astype(np.float32)
    name = (base + rise * (1 - same)) * slots + plan[:, 1:2]
    climb = plan[:, 2:3] * flip
    go_up = role_up * jnp.maximum(same, (climb == 1).astype(jnp.float32))
    go_down = role_down * jnp.maximum(same, (climb == -1).astype(jnp.float32))
    ups = go_up * (up == name)
    downs = go_down * (down == name) * level
    gap = ups + downs * strength[0][None, :]
    plus = downs * strength[1][None, :]
    straight = plan[:, 3:4] == plan[:, 4:5]
    sign = plan[:, 4:5] - plan[:, 3:4]
    return jnp.where(straight, plus, sign * gap), jnp.where(straight, plus, -sign * gap), level


def table_of(row_part, column_part, blocks, width):
    spread = np.kron(np.eye(blocks, dtype=np.float32), np.ones((1, width), np.float32))
    groups = row_part.shape[0] // blocks
    rows = row_part.reshape(groups, blocks, -1)
    wide = jnp.einsum("gea,el->gal", rows, spread, precision=HIGHEST)
    return wide + column_part.reshape(groups, 1, blocks * width)


def turned(value, steps, width):
    return value if steps == 0 else pltpu.roll(value, steps * width, 1)


def swapped(value):
    half = value.shape[1] // 2
    return jnp.concatenate([value[:, half:], value[:, :half]], 1)


def own_kernel(step, width, w_ref, other_ref, start_ref, near_ref, far_ref, right_ref, table_ref, out_ref, comm_ref):
    rows, lanes = w_ref.shape
    half = lanes // 2
    w = w_ref[...]
    left = jnp.dot(near_ref[...], w, precision=HIGHEST, preferred_element_type=jnp.float32)
    left += jnp.dot(far_ref[...], other_ref[...], precision=HIGHEST, preferred_element_type=jnp.float32)
    stacked = jnp.concatenate([w[:, :half], w[:, half:]], 0)
    right = jnp.dot(stacked, right_ref[...], precision=HIGHEST, preferred_element_type=jnp.float32)
    comm_ref[:, :half] = left[:, :half] - right[:rows]
    comm_ref[:, half:] = left[:, half:] - right[rows:]
    blocks = table_ref.shape[0]
    odd = (lax.broadcasted_iota(jnp.int32, (8, lanes), 1) // width) % 2 == 1
    for at in range(0, rows, 8):
        part = pl.ds(at, 8)
        value, comm = w_ref[part, :], comm_ref[part, :]
        total = None
        for k in range(blocks // 2):
            near = table_ref[k, part, :] * value
            far = table_ref[k + blocks // 2, part, :] * value
            if k == 1:
                near += jnp.where(odd, 0.0, -comm)
            if k + blocks // 2 == blocks - 1:
                far += jnp.where(odd, comm, 0.0)
            piece = turned(near + swapped(far), k, width)
            total = piece if total is None else total + piece
        out_ref[part, :] = start_ref[part, :] + step * total


def link_kernel(step, width, edges, *refs):
    part_ref, x_ref, z_ref, x_table, z_table = refs[:5]
    edge_refs = refs[5 : 5 + 4 * len(edges)]
    out_ref = refs[5 + 4 * len(edges)]
    edge_out = refs[6 + 4 * len(edges) :]
    rows, lanes = part_ref.shape
    half = lanes // 2
    blocks = x_table.shape[0]
    for at in range(0, rows, 8):
        part = pl.ds(at, 8)
        x, z = x_ref[part, :], z_ref[part, :]
        total = None
        for k in range(blocks // 2):
            near = x_table[k, part, :] * x + z_table[k, part, :] * z
            k_far = k + blocks // 2
            far = x_table[k_far, part, :] * x + z_table[k_far, part, :] * z
            piece = turned(near + swapped(far), k, width)
            total = piece if total is None else total + piece
        halves = [total[:, :half], total[:, half:]]
        for n, place in enumerate(edges):
            flat, slant, flat_table, slant_table = edge_refs[4 * n : 4 * n + 4]
            a, b = flat[part, :], slant[part, :]
            for k in range(blocks // 2):
                piece = flat_table[k, part, :] * a + slant_table[k, part, :] * b
                halves[place] = halves[place] + turned(piece, k, width)
        new = [part_ref[part, :half] + step * halves[0], part_ref[part, half:] + step * halves[1]]
        out_ref[part, :half] = new[0]
        out_ref[part, half:] = new[1]
        for n, place in enumerate(edges[: len(edge_out)]):
            edge_out[n][part, :] = new[place]


VMEM = pl.BlockSpec(memory_space=pltpu.VMEM)
GRANT = pltpu.CompilerParams(vmem_limit_bytes=16 * 1024 * 1024)


def shards(tiers, modes, ados, hamiltonian, couplings, rates, strength, occupancy, up_index, down_index):
    core_route, mode_routes, flat_routes, slant_routes = routes(tiers, modes)
    slots, size = ados.shape[2], hamiltonian.shape[0]
    half, lanes = size // 2, slots * 2 * size
    tier, mode = lax.axis_index("tier"), lax.axis_index("mode")
    core, chip = tier % 2, tier // 2
    turn = chip % 2
    place = core ^ turn

    def send(value, route):
        return lax.ppermute(value, AXES, route)

    own = ados.reshape(slots * 2, size, size).transpose(1, 0, 2).reshape(size, lanes)
    keep = lax.dynamic_slice(own, (core * half, 0), (half, lanes))
    got = send(lax.dynamic_slice(own, ((1 - core) * half, 0), (half, lanes)), core_route)
    first = place == 0
    start = jnp.concatenate([jnp.where(first, keep, got), jnp.where(first, got, keep)], 1)

    facts = [a.reshape(a.shape[2:]).astype(jnp.float32) for a in (occupancy, up_index, down_index)]
    info = jnp.concatenate(facts, 1)
    other_info = send(info, core_route)
    info = jnp.concatenate([jnp.where(first, info, other_info), jnp.where(first, other_info, info)], 0)
    start, info = lax.optimization_barrier((start, info))

    ham = 0.5 * (hamiltonian + hamiltonian.T)
    mine = lax.dynamic_slice(ham, (core * half, 0), (half, size))
    near = jnp.where(core == 0, mine[:, :half], mine[:, half:])
    far = jnp.where(core == 0, mine[:, half:], mine[:, :half])
    right = jnp.tile(ham, (2 * slots, 2 * slots)) * np.kron(
        np.eye(2 * slots, dtype=np.float32), np.ones((size, size), np.float32)
    )

    flip = (1 - 2 * turn).astype(jnp.float32)
    rows_c = lax.dynamic_slice(couplings, (0, core * half), (couplings.shape[0], half))
    one = jnp.float32(1.0)
    blocks = 4 * slots
    plan = block_plan(2, slots)
    sources = [(0.0, one, one)]
    for p in (0, 1):
        ahead = (mode % 2 == p).astype(jnp.float32)
        sources.append((2.0, ahead, 1.0 - ahead))
    row_w, col_w, damp = [], [], None
    for base, up, down in sources:
        a, b, level = weights_of(plan, info, base, 1.0, up, down, flip, strength, slots)
        row_w.append(a)
        col_w.append(b)
        if damp is None:
            damp = jnp.sum(level * rates[None, :], 1, keepdims=True) * plan[:, 5:6]
    row_part = jnp.dot(jnp.concatenate(row_w, 0), rows_c, precision=HIGHEST)
    row_part = jnp.concatenate([row_part[: damp.shape[0]] - damp, row_part[damp.shape[0] :]], 0)
    column_part = jnp.dot(jnp.concatenate(col_w, 0), couplings, precision=HIGHEST)
    tables = table_of(row_part, column_part, blocks, size).reshape(3, blocks, half, 2 * lanes)
    tables = [tables[0], tables[1], tables[2]]

    edge_plan = block_plan(1, slots)
    links = [p for p in (0, 1) if flat_routes[p]]
    edges = tuple(1 - p for p in links)
    edge_tables = []
    for p in links:
        lower = (chip % 2 == p) & (chip + 1 < tiers // 2)
        upper = (chip % 2 != p) & (chip >= 1)
        up, down = lower.astype(jnp.float32), upper.astype(jnp.float32)
        where = (1 - p) * slots
        pair = []
        for base in (1.0, 3.0):
            a, b, _ = weights_of(edge_plan, info[where : where + slots], base, 0.0, up, down, flip, strength, slots)
            row_part = jnp.dot(a, rows_c, precision=HIGHEST)
            column_part = jnp.dot(b, couplings, precision=HIGHEST)
            pair.append(table_of(row_part, column_part, blocks // 2, size))
        edge_tables.append(pair)

    full = jax.ShapeDtypeStruct((half, 2 * lanes), jnp.float32)
    edge = jax.ShapeDtypeStruct((half, lanes), jnp.float32)
    w = start
    brink = [start[:, q * lanes : (q + 1) * lanes] for q in edges]
    for stage in (4, 3, 2, 1):
        step = TIME_STEP / stage
        flat = [send(brink[n], flat_routes[p]) for n, p in enumerate(links)]
        slant = [send(brink[n], slant_routes[p]) for n, p in enumerate(links)]
        z = send(w, mode_routes[1])
        x = send(w, mode_routes[0])
        other = send(w, core_route)
        part = pl.pallas_call(
            functools.partial(own_kernel, step, size),
            out_shape=full,
            in_specs=[VMEM] * 7,
            out_specs=VMEM,
            scratch_shapes=[pltpu.VMEM((half, 2 * lanes), jnp.float32)],
            compiler_params=GRANT,
            name="own_part",
        )(w, other, start, near, far, right, tables[0])
        extra = [a for n in range(len(links)) for a in (flat[n], slant[n], *edge_tables[n])]
        count = len(links) if stage > 1 else 0
        result = pl.pallas_call(
            functools.partial(link_kernel, step, size, edges),
            out_shape=[full] + [edge] * count,
            in_specs=[VMEM] * (5 + len(extra)),
            out_specs=[VMEM] * (1 + count),
            compiler_params=GRANT,
            name="link_part",
        )(part, x, z, tables[1], tables[2], *extra)
        w, brink = result[0], result[1:]

    low, high = w[:, :lanes], w[:, lanes:]
    keep = jnp.where(first, low, high)
    got = send(jnp.where(first, high, low), core_route)
    whole = jnp.concatenate([jnp.where(core == 0, keep, got), jnp.where(core == 0, got, keep)], 0)
    return whole.reshape(size, slots * 2, size).transpose(1, 0, 2).reshape(ados.shape)


def solution(mesh):
    spread = P("tier", "mode", None, None)
    in_specs = (P("tier", "mode", None, None, None), P(), P(), P(), P(), spread, spread, spread)
    body = functools.partial(shards, mesh.shape["tier"], mesh.shape["mode"])
    return jax.shard_map(
        body, mesh=mesh, in_specs=in_specs, out_specs=P("tier", "mode", None, None, None), check_vma=False
    )
```

```python
import functools

import jax
import jax.numpy as jnp
import numpy as np
from jax import lax
from jax.experimental import pallas as pl
from jax.experimental.pallas import tpu as pltpu
from jax.sharding import PartitionSpec as P

TIME_STEP = 0.3
HIGHEST = lax.Precision.HIGHEST
AXES = ("tier", "mode")


def swap_pairs(pairs):
    return [route for a, b in pairs for route in ((a, b), (b, a))]


def routes(tiers, modes):
    def at(tier, mode):
        return tier * modes + mode % modes

    chips = tiers // 2
    core = [(at(2 * y, m), at(2 * y + 1, m)) for y in range(chips) for m in range(modes)]
    mode = [[(at(t, m), at(t, m + 1)) for t in range(tiers) for m in range(p, modes, 2)] for p in (0, 1)]
    flat, slant = [], []
    for p in (0, 1):
        lower = range(p, chips - 1, 2)
        flat.append([(at(2 * y + c, m), at(2 * y + 2 + c, m)) for y in lower for c in (0, 1) for m in range(modes)])
        slant.append([(at(2 * y + c, m), at(2 * y + 2 + c, m + 1)) for y in lower for c in (0, 1) for m in range(modes)])
    return (
        swap_pairs(core),
        [swap_pairs(r) for r in mode],
        [swap_pairs(r) for r in flat],
        [swap_pairs(r) for r in slant],
    )


def block_plan(groups, slots, base, rise, place):
    blocks = groups * slots * 2
    rows = []
    for k in range(blocks):
        for e in range(blocks):
            d = (e + k) % blocks
            dest, source = d // 2, e // 2
            climb = source // slots - dest // slots
            name = (base + (rise if climb else 0)) * slots + source % slots
            straight = d % 2 == e % 2
            rows.append((dest + place * slots, name, climb, 0 if straight else e % 2 - d % 2, d == e and base == 0))
    return np.array(rows, np.float32)


def setup_plan(slots, edges):
    slabs = [block_plan(2, slots, base, 1, 0) for base in (0, 2, 2)]
    for place in edges:
        slabs += [block_plan(1, slots, base, 0, place) for base in (1, 3)]
    return slabs


def turned(value, steps, width):
    return value if steps == 0 else pltpu.roll(value, steps * width, 1)


def swapped(value):
    half = value.shape[1] // 2
    return jnp.concatenate([value[:, half:], value[:, :half]], 1)


def setup_kernel(slabs, links, chips, width, plan_ref, pick_ref, info_ref, ham_ref, coup_ref, base_ref, strength_ref, *outs):
    count = len(slabs)
    tables, (ham_out, right_out), (beta_ref, wide_ref, edge_ref) = outs[:count], outs[count : count + 2], outs[count + 2 :]
    tier, mode = lax.axis_index("tier"), lax.axis_index("mode")
    core, chip = tier % 2, tier // 2
    flip = (1 - 2 * (chip % 2)).astype(jnp.float32)

    def flag(test):
        return test.astype(jnp.float32)

    roles = [(jnp.float32(1), jnp.float32(1))]
    for p in (0, 1):
        ahead = flag(mode % 2 == p)
        roles.append((ahead, 1.0 - ahead))
    for p in links:
        lower = flag((chip % 2 == p) & (chip + 1 < chips))
        upper = flag((chip % 2 != p) & (chip >= 1))
        roles += [(lower, upper), (lower, upper)]

    size = ham_ref.shape[0]
    half = size // 2
    wide = coup_ref.shape[0]
    strong, weak = strength_ref[0:1, :], strength_ref[1:2, :]
    level = jnp.dot(pick_ref[...], info_ref[0], precision=HIGHEST, preferred_element_type=jnp.float32)
    ups = jnp.dot(pick_ref[...], info_ref[1], precision=HIGHEST, preferred_element_type=jnp.float32)
    downs = jnp.dot(pick_ref[...], info_ref[2], precision=HIGHEST, preferred_element_type=jnp.float32)
    row_w, col_w = [], []
    at = 0
    for slab, (up, down) in zip(slabs, roles):
        part = slice(at, at + len(slab))
        at += len(slab)
        name, climb, sign = plan_ref[0, part, :], plan_ref[1, part, :] * flip, plan_ref[2, part, :]
        same = plan_ref[1, part, :] == 0.0
        go_up = jnp.where(same | (climb == 1.0), up, 0.0)
        go_down = jnp.where(same | (climb == -1.0), down, 0.0)
        rise = jnp.where(ups[part] == name, go_up, 0.0)
        fall = jnp.where(downs[part] == name, go_down, 0.0) * level[part]
        gap = sign * (rise + fall * strong)
        plus = fall * weak
        straight = sign == 0.0
        row_w.append(jnp.where(straight, plus, gap))
        col_w.append(jnp.where(straight, plus, -gap))
    row_w = jnp.concatenate(row_w, 0)
    drain = -plan_ref[3] * level
    mine = base_ref[pl.ds(pl.multiple_of(core * half, 8), half), :]
    contract = (((1,), (1,)), ((), ()))
    alpha = lax.dot_general(mine[:, :wide], row_w, contract, precision=HIGHEST, preferred_element_type=jnp.float32)
    alpha += lax.dot_general(mine[:, wide:], drain, contract, precision=HIGHEST, preferred_element_type=jnp.float32)
    beta_ref[...] = jnp.dot(jnp.concatenate(col_w, 0), coup_ref[...], precision=HIGHEST, preferred_element_type=jnp.float32)
    blocks = tables[0].shape[0]
    full_rows = 3 * blocks
    for e in range(blocks):
        wide_ref[:, e * width : (e + 1) * width] = beta_ref[pl.ds(e, full_rows, stride=blocks), :]
    small = blocks // 2
    edge_rows = (count - 3) * small
    first_edge = full_rows * blocks
    for e in range(small):
        if edge_rows:
            edge_ref[:, e * width : (e + 1) * width] = beta_ref[pl.ds(first_edge + e, edge_rows, stride=small), :]
    lane = lax.broadcasted_iota(jnp.int32, (8, 128), 1)
    at = 0
    for n, table in enumerate(tables):
        rolls = table.shape[0]
        for k in range(rolls):
            row = (n * blocks + k) if n < 3 else (n - 3) * small + k
            beta = wide_ref if n < 3 else edge_ref
            for a in range(0, half, 8):
                for v in range(table.shape[2] // 128):
                    e1, e2 = 128 * v // width, (128 * v + 127) // width
                    value = alpha[a : a + 8, at + e1 : at + e1 + 1]
                    if e2 > e1:
                        later = alpha[a : a + 8, at + e2 : at + e2 + 1]
                        value = jnp.where(lane < e2 * width - 128 * v, value, later)
                    table[k, a : a + 8, 128 * v : 128 * v + 128] = value + beta[row : row + 1, 128 * v : 128 * v + 128]
            at += rolls
    ham = 0.5 * (ham_ref[...] + ham_ref[...].T)
    beta_ref[0:size, :] = ham
    own = beta_ref[pl.ds(pl.multiple_of(core * half, 8), half), :]
    ham_out[...] = jnp.where(core == 0, own, jnp.concatenate([own[:, half:], own[:, :half]], 1))
    right_out[...] = jnp.zeros_like(right_out)
    for e in range(right_out.shape[0] // size):
        right_out[e * size : (e + 1) * size, e * size : (e + 1) * size] = ham


def assemble_kernel(edges, keep_ref, got_ref, out_ref, *edge_refs):
    tier = lax.axis_index("tier")
    first = ((tier % 2) ^ ((tier // 2) % 2)) == 0
    lanes = keep_ref.shape[1]
    keep, got = keep_ref[...], got_ref[...]
    halves = [jnp.where(first, keep, got), jnp.where(first, got, keep)]
    out_ref[:, :lanes] = halves[0]
    out_ref[:, lanes:] = halves[1]
    for n, place in enumerate(edges):
        edge_refs[n][...] = halves[place]


def own_kernel(step, width, w_ref, other_ref, start_ref, ham_ref, right_ref, table_ref, out_ref, comm_ref):
    rows, lanes = w_ref.shape
    half = lanes // 2
    w = w_ref[...]
    both = jnp.concatenate([w, other_ref[...]], 0)
    left = jnp.dot(ham_ref[...], both, precision=HIGHEST, preferred_element_type=jnp.float32)
    stacked = jnp.concatenate([w[:, :half], w[:, half:]], 0)
    right = jnp.dot(stacked, right_ref[...], precision=HIGHEST, preferred_element_type=jnp.float32)
    comm_ref[:, :half] = left[:, :half] - right[:rows]
    comm_ref[:, half:] = left[:, half:] - right[rows:]
    blocks = table_ref.shape[0]
    odd = (lax.broadcasted_iota(jnp.int32, (8, lanes), 1) // width) % 2 == 1
    for at in range(0, rows, 8):
        part = pl.ds(at, 8)
        value, comm = w_ref[part, :], comm_ref[part, :]
        total = None
        for k in range(blocks // 2):
            near = table_ref[k, part, :] * value
            far = table_ref[k + blocks // 2, part, :] * value
            if k == 1:
                near += jnp.where(odd, 0.0, -comm)
            if k + blocks // 2 == blocks - 1:
                far += jnp.where(odd, comm, 0.0)
            piece = turned(near + swapped(far), k, width)
            total = piece if total is None else total + piece
        out_ref[part, :] = start_ref[part, :] + step * total


def link_kernel(step, width, edges, *refs):
    part_ref, x_ref, z_ref, x_table, z_table = refs[:5]
    edge_refs = refs[5 : 5 + 4 * len(edges)]
    out_ref = refs[5 + 4 * len(edges)]
    edge_out = refs[6 + 4 * len(edges) :]
    rows, lanes = part_ref.shape
    half = lanes // 2
    blocks = x_table.shape[0]
    for at in range(0, rows, 8):
        part = pl.ds(at, 8)
        x, z = x_ref[part, :], z_ref[part, :]
        total = None
        for k in range(blocks // 2):
            near = x_table[k, part, :] * x + z_table[k, part, :] * z
            k_far = k + blocks // 2
            far = x_table[k_far, part, :] * x + z_table[k_far, part, :] * z
            piece = turned(near + swapped(far), k, width)
            total = piece if total is None else total + piece
        halves = [total[:, :half], total[:, half:]]
        for n, place in enumerate(edges):
            flat, slant, flat_table, slant_table = edge_refs[4 * n : 4 * n + 4]
            a, b = flat[part, :], slant[part, :]
            for k in range(blocks // 2):
                piece = flat_table[k, part, :] * a + slant_table[k, part, :] * b
                halves[place] = halves[place] + turned(piece, k, width)
        new = [part_ref[part, :half] + step * halves[0], part_ref[part, half:] + step * halves[1]]
        out_ref[part, :half] = new[0]
        out_ref[part, half:] = new[1]
        for n, place in enumerate(edges[: len(edge_out)]):
            edge_out[n][part, :] = new[place]


VMEM = pl.BlockSpec(memory_space=pltpu.VMEM)
GRANT = pltpu.CompilerParams(vmem_limit_bytes=16 * 1024 * 1024)


def shards(tiers, modes, ados, hamiltonian, couplings, rates, strength, occupancy, up_index, down_index):
    core_route, mode_routes, flat_routes, slant_routes = routes(tiers, modes)
    slots, size = ados.shape[2], hamiltonian.shape[0]
    half, lanes = size // 2, slots * 2 * size
    tier, mode = lax.axis_index("tier"), lax.axis_index("mode")
    core, chip = tier % 2, tier // 2
    place = core ^ (chip % 2)

    def send(value, route):
        return lax.ppermute(value, AXES, route)

    facts = jnp.stack([a.reshape(a.shape[2:]) for a in (occupancy, up_index, down_index)])
    other_facts = send(facts, core_route)
    own = ados.reshape(slots * 2, size, size).transpose(1, 0, 2).reshape(size, lanes)
    keep = lax.dynamic_slice(own, (core * half, 0), (half, lanes))
    got = send(lax.dynamic_slice(own, ((1 - core) * half, 0), (half, lanes)), core_route)
    first = place == 0
    links = [p for p in (0, 1) if flat_routes[p]]
    edges = tuple(1 - p for p in links)
    full = jax.ShapeDtypeStruct((half, 2 * lanes), jnp.float32)
    edge = jax.ShapeDtypeStruct((half, lanes), jnp.float32)
    start, *brink = pl.pallas_call(
        functools.partial(assemble_kernel, edges),
        out_shape=[full] + [edge] * len(links),
        in_specs=[VMEM] * 2,
        out_specs=[VMEM] * (1 + len(links)),
        compiler_params=GRANT,
        name="assemble",
    )(keep, got)

    late = (start, facts, other_facts, hamiltonian, couplings, rates, strength)
    start, facts, other_facts, hamiltonian, couplings, rates, strength = lax.optimization_barrier(late)
    info = jnp.concatenate([jnp.where(first, facts, other_facts), jnp.where(first, other_facts, facts)], 1)
    info = info.astype(jnp.float32)
    slabs = setup_plan(slots, edges)
    plan = np.concatenate(slabs, 0)
    bath = couplings.shape[0]
    pick = np.eye(2 * slots, dtype=np.float32)[plan[:, 0].astype(np.int32)]
    plan = np.broadcast_to(plan.T[1:, :, None], (4, plan.shape[0], bath)).copy()
    base = jnp.concatenate([couplings.T, jnp.broadcast_to(rates[None, :], (size, bath))], 1)
    blocks = 4 * slots
    big = jax.ShapeDtypeStruct((blocks, half, 2 * lanes), jnp.float32)
    small = jax.ShapeDtypeStruct((blocks // 2, half, lanes), jnp.float32)
    edge_count = 2 * len(links)
    *tables, ham, right = pl.pallas_call(
        functools.partial(setup_kernel, slabs, links, tiers // 2, size),
        out_shape=[big] * 3
        + [small] * edge_count
        + [jax.ShapeDtypeStruct((half, size), jnp.float32), jax.ShapeDtypeStruct((lanes, lanes), jnp.float32)],
        in_specs=[VMEM] * 7,
        out_specs=[VMEM] * (5 + edge_count),
        scratch_shapes=[
            pltpu.VMEM((plan.shape[1], size), jnp.float32),
            pltpu.VMEM((3 * blocks, 2 * lanes), jnp.float32),
            pltpu.VMEM((max(edge_count * blocks // 2, 8), lanes), jnp.float32),
        ],
        compiler_params=GRANT,
        name="setup",
    )(plan, pick, info, hamiltonian, couplings, base, strength)

    w = start
    for stage in (4, 3, 2, 1):
        step = TIME_STEP / stage
        flat = [send(brink[n], flat_routes[p]) for n, p in enumerate(links)]
        slant = [send(brink[n], slant_routes[p]) for n, p in enumerate(links)]
        z = send(w, mode_routes[1])
        x = send(w, mode_routes[0])
        other = send(w, core_route)
        part = pl.pallas_call(
            functools.partial(own_kernel, step, size),
            out_shape=full,
            in_specs=[VMEM] * 6,
            out_specs=VMEM,
            scratch_shapes=[pltpu.VMEM((half, 2 * lanes), jnp.float32)],
            compiler_params=GRANT,
            name="own_part",
        )(w, other, start, ham, right, tables[0])
        extra = [a for n in range(len(links)) for a in (flat[n], slant[n], *tables[3 + 2 * n : 5 + 2 * n])]
        count = len(links) if stage > 1 else 0
        result = pl.pallas_call(
            functools.partial(link_kernel, step, size, edges),
            out_shape=[full] + [edge] * count,
            in_specs=[VMEM] * (5 + len(extra)),
            out_specs=[VMEM] * (1 + count),
            compiler_params=GRANT,
            name="link_part",
        )(part, x, z, tables[1], tables[2], *extra)
        w, brink = result[0], result[1:]

    low, high = w[:, :lanes], w[:, lanes:]
    keep = jnp.where(first, low, high)
    got = send(jnp.where(first, high, low), core_route)
    whole = jnp.concatenate([jnp.where(core == 0, keep, got), jnp.where(core == 0, got, keep)], 0)
    return whole.reshape(size, slots * 2, size).transpose(1, 0, 2).reshape(ados.shape)


def solution(mesh):
    spread = P("tier", "mode", None, None)
    in_specs = (P("tier", "mode", None, None, None), P(), P(), P(), P(), spread, spread, spread)
    body = functools.partial(shards, mesh.shape["tier"], mesh.shape["mode"])
    return jax.shard_map(
        body, mesh=mesh, in_specs=in_specs, out_specs=P("tier", "mode", None, None, None), check_vma=False
    )
```

```python
import functools
import math

import jax
import jax.numpy as jnp
import numpy as np
from jax import lax
from jax.experimental import pallas as pl
from jax.experimental.pallas import tpu as pltpu
from jax.sharding import PartitionSpec as P


TIME_STEP = 0.3
HIGHEST = lax.Precision.HIGHEST
AXES = ("tier", "mode")


def swap_pairs(pairs):
    return [route for a, b in pairs for route in ((a, b), (b, a))]


def routes(tiers, modes):
    def at(tier, mode):
        return tier * modes + mode % modes

    chips = tiers // 2
    core = [(at(2 * y, m), at(2 * y + 1, m)) for y in range(chips) for m in range(modes)]
    mode = [[(at(t, m), at(t, m + 1)) for t in range(tiers) for m in range(p, modes, 2)] for p in (0, 1)]
    flat, slant = [], []
    for p in (0, 1):
        lower = range(p, chips - 1, 2)
        flat.append([(at(2 * y + c, m), at(2 * y + 2 + c, m)) for y in lower for c in (0, 1) for m in range(modes)])
        slant.append([(at(2 * y + c, m), at(2 * y + 2 + c, m + 1)) for y in lower for c in (0, 1) for m in range(modes)])
    return (
        swap_pairs(core),
        [swap_pairs(r) for r in mode],
        [swap_pairs(r) for r in flat],
        [swap_pairs(r) for r in slant],
    )


def block_plan(groups, slots, base, rise, place):
    blocks = groups * slots * 2
    rows = []
    for k in range(blocks):
        for e in range(blocks):
            d = (e + k) % blocks
            dest, source = d // 2, e // 2
            climb = source // slots - dest // slots
            name = (base + (rise if climb else 0)) * slots + source % slots
            straight = d % 2 == e % 2
            rows.append((dest + place * slots, name, climb, 0 if straight else e % 2 - d % 2, d == e and base == 0))
    return np.array(rows, np.float32)


def setup_plan(slots, edges):
    slabs = [block_plan(2, slots, base, 1, 0) for base in (0, 2, 2)]
    for place in edges:
        slabs += [block_plan(1, slots, base, 0, place) for base in (1, 3)]
    return slabs


def turned(value, steps, width):
    return value if steps == 0 else pltpu.roll(value, steps * width, 1)


def swapped(value):
    half = value.shape[1] // 2
    return jnp.concatenate([value[:, half:], value[:, :half]], 1)


def setup_kernel(slabs, links, chips, width, plan_ref, pick_ref, info_ref, ham_ref, coup_ref, rates_ref, strength_ref, *outs):
    count = len(slabs)
    tables, (ham_out, right_out), (beta_ref, wide_ref, edge_ref) = outs[:count], outs[count : count + 2], outs[count + 2 :]
    tier, mode = lax.axis_index("tier"), lax.axis_index("mode")
    core, chip = tier % 2, tier // 2
    flip = (1 - 2 * (chip % 2)).astype(jnp.float32)

    def flag(test):
        return test.astype(jnp.float32)

    roles = [(jnp.float32(1), jnp.float32(1))]
    for p in (0, 1):
        ahead = flag(mode % 2 == p)
        roles.append((ahead, 1.0 - ahead))
    for p in links:
        lower = flag((chip % 2 == p) & (chip + 1 < chips))
        upper = flag((chip % 2 != p) & (chip >= 1))
        roles += [(lower, upper), (lower, upper)]

    size = ham_ref.shape[0]
    half = size // 2
    strong, weak = strength_ref[0:1, :], strength_ref[1:2, :]
    level = jnp.dot(pick_ref[...], info_ref[0], precision=HIGHEST, preferred_element_type=jnp.float32)
    ups = jnp.dot(pick_ref[...], info_ref[1], precision=HIGHEST, preferred_element_type=jnp.float32)
    downs = jnp.dot(pick_ref[...], info_ref[2], precision=HIGHEST, preferred_element_type=jnp.float32)
    row_w, col_w = [], []
    at = 0
    for slab, (up, down) in zip(slabs, roles):
        part = slice(at, at + len(slab))
        at += len(slab)
        name, climb, sign = plan_ref[0, part, :], plan_ref[1, part, :] * flip, plan_ref[2, part, :]
        same = plan_ref[1, part, :] == 0.0
        go_up = jnp.where(same | (climb == 1.0), up, 0.0)
        go_down = jnp.where(same | (climb == -1.0), down, 0.0)
        rise = jnp.where(ups[part] == name, go_up, 0.0)
        fall = jnp.where(downs[part] == name, go_down, 0.0) * level[part]
        gap = sign * (rise + fall * strong)
        plus = fall * weak
        straight = sign == 0.0
        row_w.append(jnp.where(straight, plus, gap))
        col_w.append(jnp.where(straight, plus, -gap))
    row_w = jnp.concatenate(row_w, 0)
    drain = -plan_ref[3] * level
    turned = coup_ref[...].T
    mine = jnp.where(core == 0, turned[:half], turned[half:])
    contract = (((1,), (1,)), ((), ()))
    alpha = lax.dot_general(mine, row_w, contract, precision=HIGHEST, preferred_element_type=jnp.float32)
    every = jnp.broadcast_to(rates_ref[...], (half, rates_ref.shape[1]))
    alpha += lax.dot_general(every, drain, contract, precision=HIGHEST, preferred_element_type=jnp.float32)
    beta_ref[...] = jnp.dot(jnp.concatenate(col_w, 0), coup_ref[...], precision=HIGHEST, preferred_element_type=jnp.float32)
    blocks = tables[0].shape[0]
    full_rows = 3 * blocks
    for e in range(blocks):
        wide_ref[:, e * width : (e + 1) * width] = beta_ref[pl.ds(e, full_rows, stride=blocks), :]
    small = blocks // 2
    edge_rows = (count - 3) * small
    first_edge = full_rows * blocks
    for e in range(small):
        if edge_rows:
            edge_ref[:, e * width : (e + 1) * width] = beta_ref[pl.ds(first_edge + e, edge_rows, stride=small), :]
    lane = lax.broadcasted_iota(jnp.int32, (8, 128), 1)
    at = 0
    for n, table in enumerate(tables):
        rolls = table.shape[0]
        for k in range(rolls):
            row = (n * blocks + k) if n < 3 else (n - 3) * small + k
            beta = wide_ref if n < 3 else edge_ref
            for a in range(0, half, 8):
                for v in range(table.shape[2] // 128):
                    e1, e2 = 128 * v // width, (128 * v + 127) // width
                    value = alpha[a : a + 8, at + e1 : at + e1 + 1]
                    if e2 > e1:
                        later = alpha[a : a + 8, at + e2 : at + e2 + 1]
                        value = jnp.where(lane < e2 * width - 128 * v, value, later)
                    table[k, a : a + 8, 128 * v : 128 * v + 128] = value + beta[row : row + 1, 128 * v : 128 * v + 128]
            at += rolls
    ham = 0.5 * (ham_ref[...] + ham_ref[...].T)
    beta_ref[0:size, :] = ham
    own = beta_ref[pl.ds(pl.multiple_of(core * half, 8), half), :]
    ham_out[...] = jnp.where(core == 0, own, jnp.concatenate([own[:, half:], own[:, :half]], 1))
    right_out[...] = jnp.zeros_like(right_out)
    for e in range(right_out.shape[0] // size):
        right_out[e * size : (e + 1) * size, e * size : (e + 1) * size] = ham


def split_kernel(count, *refs):
    sources, (keep_ref, send_ref, facts_ref), copies = refs[:count], refs[count : count + 3], refs[count + 3 : 2 * count - 1]
    raw_ref, lines_ref, rows_ref, sems = refs[2 * count - 1 :]
    targets = [raw_ref] + [facts_ref.at[n] for n in range(3)] + list(copies)
    moves = [pltpu.make_async_copy(a, b, sems.at[n]) for n, (a, b) in enumerate(zip(sources, targets))]
    for move in moves:
        move.start()
    moves[0].wait()
    core = lax.axis_index("tier") % 2
    half, lanes = keep_ref.shape
    size, (turns, groups, _) = 2 * half, lines_ref.shape
    lines = size * turns // 128
    for s in range(raw_ref.shape[0]):
        for part in (0, 1):
            flat = [raw_ref[s, pl.ds(2 * p + part, groups, stride=2 * lines), :] for p in range(lines)]
            flat = jnp.concatenate(flat, 1)
            block = (2 * s + part) * size
            for q in range(turns):
                lines_ref[q, :, block : block + size] = flat[:, q * size : (q + 1) * size]
    for v in range(lanes // 128):
        at = slice(128 * v, 128 * v + 128)
        for q in range(turns):
            rows_ref[v, pl.ds(q, groups, stride=turns), :] = lines_ref[q, :, at]
        keep_ref[:, at] = rows_ref[v, pl.ds(pl.multiple_of(core * half, 8), half), :]
        send_ref[:, at] = rows_ref[v, pl.ds(pl.multiple_of((1 - core) * half, 8), half), :]
    for move in moves[1:]:
        move.wait()


def assemble_kernel(edges, keep_ref, got_ref, facts_ref, other_ref, out_ref, info_ref, *edge_refs):
    tier = lax.axis_index("tier")
    first = ((tier % 2) ^ ((tier // 2) % 2)) == 0
    lanes = keep_ref.shape[1]
    keep, got = keep_ref[...], got_ref[...]
    halves = [jnp.where(first, keep, got), jnp.where(first, got, keep)]
    out_ref[:, :lanes] = halves[0]
    out_ref[:, lanes:] = halves[1]
    for n, place in enumerate(edges):
        edge_refs[n][...] = halves[place]
    slots = facts_ref.shape[1]
    for n in range(3):
        mine, other = facts_ref[n].astype(jnp.float32), other_ref[n].astype(jnp.float32)
        info_ref[n, :slots, :] = jnp.where(first, mine, other)
        info_ref[n, slots:, :] = jnp.where(first, other, mine)


def finish_kernel(keep_ref, got_ref, out_ref, rows_ref, lines_ref):
    upper = lax.axis_index("tier") % 2 == 0
    half = keep_ref.shape[0]
    size, (groups, length) = 2 * half, lines_ref.shape[1:]
    turns, lines = length // size, length // 128
    planes = rows_ref.shape[0]
    for v in range(planes):
        at = slice(128 * v, 128 * v + 128)
        keep, got = keep_ref[:, at], got_ref[:, at]
        rows_ref[v, :half] = jnp.where(upper, keep, got)
        rows_ref[v, half:] = jnp.where(upper, got, keep)
    rows = [[rows_ref[v, pl.ds(q, groups, stride=turns), :] for v in range(planes)] for q in range(turns)]
    rows = [jnp.concatenate(r, 1) for r in rows]
    for s in range(out_ref.shape[0]):
        for part in (0, 1):
            block = 2 * s + part
            for q in range(turns):
                lines_ref[block, :, q * size : (q + 1) * size] = rows[q][:, block * size : (block + 1) * size]
            for p in range(lines):
                out_ref[s, pl.ds(2 * p + part, groups, stride=2 * lines), :] = lines_ref[block, :, 128 * p : 128 * (p + 1)]


def own_kernel(step, width, w_ref, start_ref, right_ref, table_ref, out_ref, right_out):
    rows, lanes = w_ref.shape
    half = lanes // 2
    stacked = jnp.concatenate([w_ref[:, :half], w_ref[:, half:]], 0)
    right = jnp.dot(stacked, right_ref[...], precision=HIGHEST, preferred_element_type=jnp.float32)
    right_out[:, :half] = right[:rows]
    right_out[:, half:] = right[rows:]
    blocks = table_ref.shape[0]
    for at in range(0, rows, 8):
        part = pl.ds(at, 8)
        value = w_ref[part, :]
        total = None
        for k in range(blocks // 2):
            near, far = table_ref[k, part, :] * value, table_ref[k + blocks // 2, part, :] * value
            piece = turned(near + swapped(far), k, width)
            total = piece if total is None else total + piece
        out_ref[part, :] = start_ref[part, :] + step * total


def left_kernel(step, width, w_ref, other_ref, ham_ref, part_ref, right_ref, out_ref, comm_ref):
    rows, lanes = w_ref.shape
    both = jnp.concatenate([w_ref[...], other_ref[...]], 0)
    comm_ref[...] = jnp.dot(ham_ref[...], both, precision=HIGHEST, preferred_element_type=jnp.float32)
    odd = (lax.broadcasted_iota(jnp.int32, (8, lanes), 1) // width) % 2 == 1
    for at in range(0, rows, 8):
        part = pl.ds(at, 8)
        comm = step * (comm_ref[part, :] - right_ref[part, :])
        real = pltpu.roll(jnp.where(odd, comm, 0.0), lanes - width, 1)
        imag = pltpu.roll(jnp.where(odd, 0.0, comm), width, 1)
        out_ref[part, :] = part_ref[part, :] + (real - imag)


def link_kernel(step, width, edges, last, *refs):
    part_ref, x_ref, z_ref, x_table, z_table = refs[:5]
    edge_refs = refs[5 : 5 + 4 * len(edges)]
    outs = refs[5 + 4 * len(edges) :]
    tier = lax.axis_index("tier")
    first = ((tier % 2) ^ ((tier // 2) % 2)) == 0
    rows, lanes = part_ref.shape
    half = lanes // 2
    blocks = x_table.shape[0]
    for at in range(0, rows, 8):
        part = pl.ds(at, 8)
        x, z = x_ref[part, :], z_ref[part, :]
        total = None
        for k in range(blocks // 2):
            near = x_table[k, part, :] * x + z_table[k, part, :] * z
            k_far = k + blocks // 2
            far = x_table[k_far, part, :] * x + z_table[k_far, part, :] * z
            piece = turned(near + swapped(far), k, width)
            total = piece if total is None else total + piece
        halves = [total[:, :half], total[:, half:]]
        for n, place in enumerate(edges):
            flat, slant, flat_table, slant_table = edge_refs[4 * n : 4 * n + 4]
            a, b = flat[part, :], slant[part, :]
            for k in range(blocks // 2):
                piece = flat_table[k, part, :] * a + slant_table[k, part, :] * b
                halves[place] = halves[place] + turned(piece, k, width)
        new = [part_ref[part, :half] + step * halves[0], part_ref[part, half:] + step * halves[1]]
        if last:
            outs[0][part, :] = jnp.where(first, new[0], new[1])
            outs[1][part, :] = jnp.where(first, new[1], new[0])
            continue
        outs[0][part, :half] = new[0]
        outs[0][part, half:] = new[1]
        for n, place in enumerate(edges):
            outs[1 + n][part, :] = new[place]


VMEM = pl.BlockSpec(memory_space=pltpu.VMEM)
GRANT = pltpu.CompilerParams(vmem_limit_bytes=16 * 1024 * 1024)


def shards(tiers, modes, ados, hamiltonian, couplings, rates, strength, occupancy, up_index, down_index):
    core_route, mode_routes, flat_routes, slant_routes = routes(tiers, modes)
    slots, size = ados.shape[2], hamiltonian.shape[0]
    half, lanes = size // 2, slots * 2 * size

    def send(value, route):
        return lax.ppermute(value, AXES, route)

    turns = 128 // math.gcd(size, 128)
    groups, count = size // turns, size * size // 128
    raw = ados.reshape(slots, 2, count, 128).transpose(0, 2, 1, 3).reshape(slots, 2 * count, 128)
    edge = jax.ShapeDtypeStruct((half, lanes), jnp.float32)
    full = jax.ShapeDtypeStruct((half, 2 * lanes), jnp.float32)
    links = [p for p in (0, 1) if flat_routes[p]]
    edges = tuple(1 - p for p in links)
    bath = couplings.shape[0]
    slabs = setup_plan(slots, edges)
    plan = np.concatenate(slabs, 0)
    pick = np.eye(2 * slots, dtype=np.float32)[plan[:, 0].astype(np.int32)]
    plan = np.broadcast_to(plan.T[1:, :, None], (4, plan.shape[0], bath)).copy()
    index = [a.reshape(slots, bath) for a in (occupancy, up_index, down_index)]
    small = [hamiltonian, couplings, rates.reshape(1, bath), strength, plan, pick]
    count_in = 4 + len(small)
    keep, away, facts, *small = pl.pallas_call(
        functools.partial(split_kernel, count_in),
        out_shape=[edge, edge, jax.ShapeDtypeStruct((3, slots, bath), jnp.int32)]
        + [jax.ShapeDtypeStruct(a.shape, jnp.float32) for a in small],
        in_specs=[pl.BlockSpec(memory_space=pltpu.HBM)] * count_in,
        out_specs=[VMEM] * (3 + len(small)),
        scratch_shapes=[
            pltpu.VMEM(raw.shape, jnp.float32),
            pltpu.VMEM((turns, groups, lanes), jnp.float32),
            pltpu.VMEM((lanes // 128, size, 128), jnp.float32),
            pltpu.SemaphoreType.DMA((count_in,)),
        ],
        compiler_params=GRANT,
        name="split",
    )(*[pltpu.with_memory_space_constraint(jnp.asarray(a), pltpu.HBM) for a in (raw, *index, *small)])
    other_facts = send(facts, core_route)
    got = send(away, core_route)
    start, info, *brink = pl.pallas_call(
        functools.partial(assemble_kernel, edges),
        out_shape=[full, jax.ShapeDtypeStruct((3, 2 * slots, bath), jnp.float32)] + [edge] * len(links),
        in_specs=[VMEM] * 4,
        out_specs=[VMEM] * (2 + len(links)),
        compiler_params=GRANT,
        name="assemble",
    )(keep, got, facts, other_facts)

    start, info, small = lax.optimization_barrier((start, info, small))
    hamiltonian, couplings, rates, strength, plan, pick = small
    blocks = 4 * slots
    big = jax.ShapeDtypeStruct((blocks, half, 2 * lanes), jnp.float32)
    narrow = jax.ShapeDtypeStruct((blocks // 2, half, lanes), jnp.float32)
    edge_count = 2 * len(links)
    *tables, ham, right = pl.pallas_call(
        functools.partial(setup_kernel, slabs, links, tiers // 2, size),
        out_shape=[big] * 3
        + [narrow] * edge_count
        + [jax.ShapeDtypeStruct((half, size), jnp.float32), jax.ShapeDtypeStruct((lanes, lanes), jnp.float32)],
        in_specs=[VMEM] * 7,
        out_specs=[VMEM] * (5 + edge_count),
        scratch_shapes=[
            pltpu.VMEM((plan.shape[1], size), jnp.float32),
            pltpu.VMEM((3 * blocks, 2 * lanes), jnp.float32),
            pltpu.VMEM((max(edge_count * blocks // 2, 8), lanes), jnp.float32),
        ],
        compiler_params=GRANT,
        name="setup",
    )(plan, pick, info, hamiltonian, couplings, rates, strength)

    w = start
    for stage in (4, 3, 2, 1):
        step = TIME_STEP / stage
        flat = [send(brink[n], flat_routes[p]) for n, p in enumerate(links)]
        slant = [send(brink[n], slant_routes[p]) for n, p in enumerate(links)]
        z = send(w, mode_routes[1])
        x = send(w, mode_routes[0])
        other = send(w, core_route)
        part, product = pl.pallas_call(
            functools.partial(own_kernel, step, size),
            out_shape=[full, full],
            in_specs=[VMEM] * 4,
            out_specs=[VMEM] * 2,
            compiler_params=GRANT,
            name="own_part",
        )(w, start, right, tables[0])
        part = pl.pallas_call(
            functools.partial(left_kernel, step, size),
            out_shape=full,
            in_specs=[VMEM] * 5,
            out_specs=VMEM,
            scratch_shapes=[pltpu.VMEM((half, 2 * lanes), jnp.float32)],
            compiler_params=GRANT,
            name="left_part",
        )(w, other, ham, part, product)
        extra = [a for n in range(len(links)) for a in (flat[n], slant[n], *tables[3 + 2 * n : 5 + 2 * n])]
        last = stage == 1
        shapes = [edge] * 2 if last else [full] + [edge] * len(links)
        w, *brink = pl.pallas_call(
            functools.partial(link_kernel, step, size, edges, last),
            out_shape=shapes,
            in_specs=[VMEM] * (5 + len(extra)),
            out_specs=[VMEM] * len(shapes),
            compiler_params=GRANT,
            name="link_part",
        )(part, x, z, tables[1], tables[2], *extra)

    out = pl.pallas_call(
        finish_kernel,
        out_shape=jax.ShapeDtypeStruct(raw.shape, jnp.float32),
        in_specs=[VMEM] * 2,
        out_specs=VMEM,
        scratch_shapes=[pltpu.VMEM((lanes // 128, size, 128), jnp.float32), pltpu.VMEM((2 * slots, groups, turns * size), jnp.float32)],
        compiler_params=GRANT,
        name="finish",
    )(w, send(brink[0], core_route))
    return out.reshape(slots, count, 2, 128).transpose(0, 2, 1, 3).reshape(ados.shape)


def solution(mesh):
    spread = P("tier", "mode", None, None)
    in_specs = (P("tier", "mode", None, None, None), P(), P(), P(), P(), spread, spread, spread)
    body = functools.partial(shards, mesh.shape["tier"], mesh.shape["mode"])
    return jax.shard_map(
        body, mesh=mesh, in_specs=in_specs, out_specs=P("tier", "mode", None, None, None), check_vma=False
    )
```
